32 devices in a mesh: dp: 4 (over y, core), ctx: 8 (over z, x).
Axes of the slice: x: 2, y: 2, z: 4, core: 2. Of those that a mesh axis runs over, the one named last changes fastest.
Arguments:
- text: bfloat16 [4, 2, 128, 2048], P('dp', None, None, 'ctx'), may hold values from -6 to 6
- src: int32 [4], replicated, may hold values from 0 to 3, each once
- lengths: int32 [4, 2], replicated, may hold values from 1 to 128
- kv_weight: bfloat16 [2048, 2, 8192], P('dp', None, 'ctx'), may hold values from -0.125 to 0.125
- queries: bfloat16 [4, 2048, 4096], P('dp', 'ctx'), may hold values from -160 to 160
- grad_out: bfloat16 [4, 2048, 4096], P('dp', 'ctx'), may hold values from -6 to 6
Outputs:
- attended: bfloat16 [4, 2048, 4096], P('dp', 'ctx')
- grad_queries: bfloat16 [4, 2048, 4096], P('dp', 'ctx')
- grad_weight: float32 [2048, 2, 8192], P('dp', None, 'ctx')
The draws below stay inside these ranges and needn't reach their ends.
Inputs may be any that keep to these rules, and one draw needn't show every extreme that they name: `src`: each text sample is used by exactly one latent sample. `lengths`: tokens of an encoder output at or beyond its length are padding.
All inputs are finite; a program needn't handle non-finite values.
Results may differ from the reference program's by a relative error of at most 0.018.
The reference program's roundings to bfloat16 on the way count: a program that leaves them out, or rounds other values in their place, can miss the bound.
Values may be sent and summed in bfloat16 or wider, within the bound.
A program may use at most 128 MiB of HBM per device.

```python
import math
import jax
import jax.numpy as jnp
from jax import lax

HEAD = 128
E = 2048
TT = 128
HD = 4096
SAMPLES = 4
LAT = 2048


def draw_queries(key, part):
    base = jax.random.normal(jax.random.fold_in(key, 11), (SAMPLES, LAT, HD), jnp.float32)
    base = jnp.clip(base, -6.0, 6.0)
    return base.astype(jnp.bfloat16)


def set_ends(values, stream_key, smallest, largest):
    longest = values.shape.index(max(values.shape))
    spots = []
    for shift in (0, 1):
        where = [jax.random.randint(jax.random.fold_in(stream_key, axis), (), 0, length) for axis, length in enumerate(values.shape)]
        where[longest] = (where[longest] + shift) % values.shape[longest]
        spots.append(tuple(where))
    return values.at[spots[0]].set(smallest).at[spots[1]].set(largest)


def steps_of(stream_key, shape, split, smallest, top_value):
    def one(axis_at, blocks):
        heights = jax.random.uniform(jax.random.fold_in(jax.random.fold_in(stream_key, 6), axis_at), (blocks,), jnp.float32, smallest / len(split), top_value / len(split))
        return jnp.repeat(jnp.exp(heights), shape[axis_at] // blocks).reshape((-1,) + (1,) * (len(shape) - axis_at - 1))

    gain = one(*split[0])
    for cut in split[1:]:
        gain = gain * one(*cut)
    return gain


def noise(own_key, shape, scale, reach, pieces=(), kind=jnp.bfloat16):
    entries = scale * jax.random.normal(own_key, shape, jnp.float32)
    if pieces:
        entries = entries * steps_of(own_key, shape, pieces, -0.22, 0.18)
    return jnp.clip(entries, -reach, reach).astype(kind)


def setup_inputs(seed: int = 0) -> dict:
    streams_of = jax.random.split(jax.random.key(seed), 7)
    return {
        "text": noise(streams_of[0], (SAMPLES, 2, TT, E), 1.0, 6.0, ((0, 4), (3, 8))),
        "src": jax.random.permutation(streams_of[1], SAMPLES).astype(jnp.int32),
        "lengths": set_ends(jax.random.randint(streams_of[2], (SAMPLES, 2), 1, TT + 1), jax.random.fold_in(streams_of[2], 1), 1, TT).astype(jnp.int32),
        "kv_weight": noise(streams_of[3], (E, 2, 2 * HD), E ** -0.5, 0.125, ((0, 4), (2, 8))),
        "queries": draw_queries(jax.random.fold_in(streams_of[6], 71), 0),
        "grad_out": noise(streams_of[5], (SAMPLES, LAT, HD), 1.0, 6.0, ((0, 4), (1, 8))),
    }


def attend_one(query, key_value, valid, cotangent):
    length = query.shape[0]
    heads = query.shape[1] // HEAD
    keys = key_value.shape[0] * key_value.shape[1]
    scale = 1.0 / math.sqrt(HEAD)
    paired = key_value.reshape(keys, heads, 2, HEAD).astype(jnp.float32)
    key = paired[:, :, 0]
    value = paired[:, :, 1]
    q_rows = query.reshape(length, heads, HEAD).astype(jnp.float32)
    g_rows = cotangent.reshape(length, heads, HEAD).astype(jnp.float32)
    scores = jnp.einsum('lhd,jhd->hlj', q_rows, key) * scale
    scores = jnp.where(valid[None, None, :], scores, -1e+30)
    top = lax.optimization_barrier(jnp.max(scores, axis=-1, keepdims=True))
    weights = jnp.exp(scores - top)
    probs = weights / lax.optimization_barrier(jnp.sum(weights, axis=-1, keepdims=True))
    probs_low = lax.optimization_barrier(probs.astype(jnp.bfloat16)).astype(jnp.float32)
    attended = jnp.einsum('hlj,jhd->lhd', probs_low, value).reshape(length, heads * HEAD).astype(jnp.bfloat16)
    grad_probs = jnp.einsum('lhd,jhd->hlj', g_rows, value)
    delta = lax.optimization_barrier(jnp.sum(probs * grad_probs, axis=-1, keepdims=True))
    grad_scores = (probs * (grad_probs - delta) * scale).astype(jnp.bfloat16)
    grad_scores = lax.optimization_barrier(grad_scores).astype(jnp.float32)
    grad_queries = jnp.einsum('hlj,jhd->lhd', grad_scores, key).reshape(length, heads * HEAD).astype(jnp.bfloat16)
    grad_key = jnp.einsum('hlj,lhd->jhd', grad_scores, q_rows)
    grad_value = jnp.einsum('hlj,lhd->jhd', probs_low, g_rows)
    grad_kv = jnp.stack([grad_key, grad_value], axis=2).reshape(2, keys // 2, heads * 2 * HEAD)
    return (attended, grad_queries, grad_kv)

def reference(text, src, lengths, kv_weight, queries, grad_out):
    ctx_text = jnp.take(text, src.astype(jnp.int32), axis=0)
    wide_text = ctx_text.astype(jnp.float32)
    kv = jnp.einsum('betf,fec->betc', wide_text, kv_weight.astype(jnp.float32)).astype(jnp.bfloat16)
    chosen = jnp.take(lengths, src.astype(jnp.int32), axis=0)
    positions = jnp.arange(TT, dtype=jnp.int32)
    valid = (positions[None, None, :] < chosen[:, :, None]).reshape(SAMPLES, 2 * TT)

    def one_sample(items):
        return attend_one(items[0], items[1], items[2], items[3])
    attended, grad_queries, grad_kv = lax.map(one_sample, (queries, kv, valid, grad_out))
    grad_low = lax.optimization_barrier(grad_kv.astype(jnp.bfloat16)).astype(jnp.float32)
    grad_weight = jnp.einsum('betf,betc->fec', wide_text, grad_low)
    return (attended, grad_queries, grad_weight)
```

```python
import functools
import math

import jax
import jax.numpy as jnp
from jax import lax
from jax.experimental import pallas as pl
from jax.experimental.pallas import tpu as pltpu
from jax.sharding import PartitionSpec as P

HEAD = 128


def dot(a, b, dims):
    return lax.dot_general(a, b, (dims, ((), ())), preferred_element_type=jnp.float32)


def attend_kernel(heads, bias_ref, q_ref, g_ref, kv_ref, out_ref, gq_ref, gkv_ref):
    scale = 1.0 / math.sqrt(HEAD)
    bias = bias_ref[...]
    for h in range(heads):
        own = slice(h * HEAD, (h + 1) * HEAD)
        at_key = slice(2 * h * HEAD, (2 * h + 1) * HEAD)
        at_value = slice((2 * h + 1) * HEAD, (2 * h + 2) * HEAD)
        q = q_ref[:, own]
        g = g_ref[:, own]
        key = kv_ref[0, :, at_key]
        value = kv_ref[0, :, at_value]
        scores = dot(q, key, ((1,), (1,))) * scale + bias
        top = jnp.max(scores, axis=-1, keepdims=True)
        weights = jnp.exp(scores - top)
        probs = weights * (1.0 / jnp.sum(weights, axis=-1, keepdims=True))
        probs_low = probs.astype(jnp.bfloat16)
        out_ref[:, own] = dot(probs_low, value, ((1,), (0,))).astype(jnp.bfloat16)
        grad_probs = dot(g, value, ((1,), (1,)))
        delta = jnp.sum(probs * grad_probs, axis=-1, keepdims=True)
        grad_scores = (probs * (grad_probs - delta) * scale).astype(jnp.bfloat16)
        gq_ref[:, own] = dot(grad_scores, key, ((1,), (0,))).astype(jnp.bfloat16)
        gkv_ref[0, :, at_key] = dot(grad_scores, q, ((0,), (0,))).astype(gkv_ref.dtype)
        gkv_ref[0, :, at_value] = dot(probs_low, g, ((0,), (0,))).astype(gkv_ref.dtype)


def attend(bias, queries, grad_out, kv):
    length, width = queries.shape
    blocks, keys, columns = kv.shape
    per_block = columns // (2 * HEAD)
    heads = math.gcd(per_block, 4)
    steps = per_block // heads
    rows = pl.BlockSpec((length, heads * HEAD), lambda i, j: (0, i * steps + j))
    pairs = pl.BlockSpec((1, keys, heads * 2 * HEAD), lambda i, j: (i, 0, j))
    flops = 12 * length * keys * width
    return pl.pallas_call(
        functools.partial(attend_kernel, heads),
        grid=(blocks, steps),
        in_specs=[pl.BlockSpec((1, keys), lambda i, j: (0, 0)), rows, rows, pairs],
        out_specs=[rows, rows, pairs],
        out_shape=[
            jax.ShapeDtypeStruct(queries.shape, jnp.bfloat16),
            jax.ShapeDtypeStruct(queries.shape, jnp.bfloat16),
            jax.ShapeDtypeStruct(kv.shape, jnp.bfloat16),
        ],
        cost_estimate=pl.CostEstimate(
            flops=flops, bytes_accessed=2 * (4 * length * width + 2 * kv.size), transcendentals=length * keys * width // HEAD
        ),
        name="attend",
    )(bias, queries, grad_out, kv)


def greet(axis, a, last, up, down, partner):
    barrier = pltpu.get_barrier_semaphore()

    def hello(target):
        pl.semaphore_signal(barrier, inc=1, device_id={axis: target}, device_id_type=pl.DeviceIdType.MESH)

    hello(partner)

    @pl.when(a < last)
    def _():
        hello(up)

    @pl.when(a > 0)
    def _():
        hello(down)

    if last == 0:
        pl.semaphore_wait(barrier, 1)
    else:
        @pl.when((a > 0) & (a < last))
        def _():
            pl.semaphore_wait(barrier, 3)

        @pl.when((a == 0) | (a == last))
        def _():
            pl.semaphore_wait(barrier, 2)


def gather_kernel(axis, n, own_ref, out_ref, own_sem, send_sems, recv_sems):
    me = lax.axis_index(axis)
    a, b = me // 2, me % 2
    last = n // 2 - 1
    up, down, partner = me + 2, me - 2, a * 2 + (1 - b)
    greet(axis, a, last, up, down, partner)
    mine = pltpu.make_async_copy(own_ref, out_ref.at[me], own_sem)
    mine.start()

    def hop(source, block, way, target):
        return pltpu.make_async_remote_copy(
            src_ref=source, dst_ref=out_ref.at[block], send_sem=send_sems.at[block, way],
            recv_sem=recv_sems.at[block], device_id={axis: target}, device_id_type=pl.DeviceIdType.MESH,
        )

    @pl.when(a < last)
    def _():
        hop(own_ref, me, 0, up).start()

    @pl.when(a > 0)
    def _():
        hop(own_ref, me, 1, down).start()

    hop(own_ref, me, 2, partner).start()
    for s in range(1, last + 1):
        @pl.when(a >= s)
        def _():
            block = (a - s) * 2 + b
            hop(own_ref, block, 0, partner).wait_recv()

            @pl.when(a < last)
            def _():
                hop(out_ref.at[block], block, 0, up).start()

            hop(out_ref.at[block], block, 2, partner).start()

        @pl.when(a + s <= last)
        def _():
            block = (a + s) * 2 + b
            hop(own_ref, block, 1, partner).wait_recv()

            @pl.when(a > 0)
            def _():
                hop(out_ref.at[block], block, 1, down).start()

            hop(out_ref.at[block], block, 2, partner).start()

    for z in range(last + 1):
        hop(own_ref, z * 2 + 1 - b, 2, partner).wait_recv()
        hop(own_ref, z * 2 + b, 2, partner).wait_send()

        @pl.when((a < last) & (a >= z))
        def _():
            hop(own_ref, z * 2 + b, 0, partner).wait_send()

        @pl.when((a > 0) & (a <= z))
        def _():
            hop(own_ref, z * 2 + b, 1, partner).wait_send()

    mine.wait()


def gather(block, axis, n, collective_id):
    return pl.pallas_call(
        functools.partial(gather_kernel, axis, n),
        in_specs=[pl.BlockSpec(memory_space=pltpu.VMEM)],
        out_specs=pl.BlockSpec(memory_space=pl.ANY),
        out_shape=jax.ShapeDtypeStruct((n,) + block.shape, block.dtype),
        scratch_shapes=[
            pltpu.SemaphoreType.DMA,
            pltpu.SemaphoreType.DMA((n, 3)),
            pltpu.SemaphoreType.DMA((n,)),
        ],
        compiler_params=pltpu.CompilerParams(collective_id=collective_id, has_side_effects=True),
        name="gather",
    )(block)


def scatter_kernel(axis, n, g_ref, out_ref, crossed, risen, fallen, going, send_sems, x_sems, up_sems, down_sems):
    me = lax.axis_index(axis)
    a, b = me // 2, me % 2
    last = n // 2 - 1
    up, down, partner = me + 2, me - 2, a * 2 + (1 - b)
    greet(axis, a, last, up, down, partner)
    rows = out_ref.shape[0]
    step = min(rows, 32)
    half = (last + 2) // 2
    high = a // half

    def place(t):
        return high * t + (1 - high) * (last - t)

    def cross(z):
        return pltpu.make_async_remote_copy(
            src_ref=g_ref.at[z * 2 + 1 - b], dst_ref=crossed.at[z], send_sem=send_sems.at[z, 0],
            recv_sem=x_sems.at[z], device_id={axis: partner}, device_id_type=pl.DeviceIdType.MESH,
        )

    def rise(z):
        return pltpu.make_async_remote_copy(
            src_ref=going.at[z], dst_ref=risen.at[z], send_sem=send_sems.at[z, 1],
            recv_sem=up_sems.at[z], device_id={axis: up}, device_id_type=pl.DeviceIdType.MESH,
        )

    def fall(z):
        return pltpu.make_async_remote_copy(
            src_ref=going.at[z], dst_ref=fallen.at[z], send_sem=send_sems.at[z, 2],
            recv_sem=down_sems.at[z], device_id={axis: down}, device_id_type=pl.DeviceIdType.MESH,
        )

    def add(target, parts):
        @pl.loop(0, rows // step)
        def _(i):
            at = pl.ds(pl.multiple_of(i * step, step), step)
            total = parts[0][at, :].astype(jnp.float32)
            for part in parts[1:]:
                total = total + part[at, :].astype(jnp.float32)
            target[at, :] = total.astype(target.dtype)

    for t in range(last + 1):
        cross(place(t)).start()
    for t in range(last + 1):
        z = place(t)
        cross(z).wait_recv()
        pair = [g_ref.at[z * 2 + b], crossed.at[z]]

        @pl.when(z > a)
        def _():
            @pl.when(a > 0)
            def _():
                rise(z).wait_recv()
                add(going.at[z], pair + [risen.at[z]])

            @pl.when(a == 0)
            def _():
                add(going.at[z], pair)

            rise(z).start()

        @pl.when(z < a)
        def _():
            @pl.when(a < last)
            def _():
                fall(z).wait_recv()
                add(going.at[z], pair + [fallen.at[z]])

            @pl.when(a == last)
            def _():
                add(going.at[z], pair)

            fall(z).start()

    pair = [g_ref.at[a * 2 + b], crossed.at[a]]

    @pl.when(a > 0)
    def _():
        rise(a).wait_recv()

    @pl.when(a < last)
    def _():
        fall(a).wait_recv()

    @pl.when(a == 0)
    def _():
        add(out_ref, pair + [fallen.at[a]])

    @pl.when(a == last)
    def _():
        add(out_ref, pair + [risen.at[a]])

    @pl.when((a > 0) & (a < last))
    def _():
        add(out_ref, pair + [risen.at[a], fallen.at[a]])

    for z in range(last + 1):
        cross(z).wait_send()

        @pl.when(z > a)
        def _():
            rise(z).wait_send()

        @pl.when(z < a)
        def _():
            fall(z).wait_send()


def scatter(parts, axis, collective_id):
    n, rows, columns = parts.shape
    half = n // 2
    blocks = pltpu.VMEM((half, rows, columns), parts.dtype)
    return pl.pallas_call(
        functools.partial(scatter_kernel, axis, n),
        in_specs=[pl.BlockSpec(memory_space=pltpu.VMEM)],
        out_specs=pl.BlockSpec(memory_space=pltpu.VMEM),
        out_shape=jax.ShapeDtypeStruct((rows, columns), jnp.bfloat16),
        scratch_shapes=[blocks] * 4
        + [
            pltpu.SemaphoreType.DMA((half, 3)),
            pltpu.SemaphoreType.DMA((half,)),
            pltpu.SemaphoreType.DMA((half,)),
            pltpu.SemaphoreType.DMA((half,)),
        ],
        compiler_params=pltpu.CompilerParams(
            collective_id=collective_id, has_side_effects=True, vmem_limit_bytes=40 << 20
        ),
        name="scatter",
    )(parts)


def per_device(groups, text, src, lengths, kv_weight, queries, grad_out):
    dp, ctx = groups
    group = lax.axis_index("dp")
    samples = src.shape[0]
    share = ctx // dp
    tokens = text.shape[2]
    keys = 2 * tokens
    features = kv_weight.shape[0]
    columns = kv_weight.shape[2]
    hops = [
        (d * ctx + c, (c // share) * ctx + d * share + c % share)
        for d in range(dp)
        for c in range(ctx)
    ]
    mine = lax.ppermute(text[0], ("dp", "ctx"), hops)
    pieces = gather(mine.reshape(2 * tokens, -1), "ctx", ctx, 1)
    pieces = pieces.reshape(samples, share, 2, tokens, features // share)
    by_text = jnp.transpose(pieces, (0, 2, 3, 1, 4)).reshape(samples, 2, tokens, features)
    rows = jnp.stack(
        [lax.dynamic_index_in_dim(by_text, src[b], 0, keepdims=False) for b in range(samples)]
    )
    partial = jnp.einsum("betf,fec->betc", rows, kv_weight, preferred_element_type=jnp.float32)
    kv_local = scatter(partial.reshape(samples, keys, columns), "dp", 4)
    kv = gather(kv_local, "ctx", ctx, 2)
    own_lengths = lax.dynamic_index_in_dim(lengths, src[group], 0, keepdims=False)
    valid = jnp.arange(tokens, dtype=jnp.int32)[None, :] < own_lengths[:, None]
    bias = jnp.where(valid, 0.0, -1e30).astype(jnp.float32).reshape(1, keys)
    attended, grad_queries, grad_kv = attend(bias, queries[0], grad_out[0], kv)
    grad_low = scatter(grad_kv, "ctx", 3)
    grads = gather(grad_low, "dp", dp, 5)
    grads = grads.reshape(samples, 2, tokens, columns)
    grad_weight = jnp.einsum("betf,betc->fec", rows, grads, preferred_element_type=jnp.float32)
    return (attended[None], grad_queries[None], grad_weight)


def solution(mesh):
    placed = (
        P("dp", None, None, "ctx"),
        P(),
        P(),
        P("dp", None, "ctx"),
        P("dp", "ctx", None),
        P("dp", "ctx", None),
    )
    return jax.shard_map(
        functools.partial(per_device, (mesh.shape["dp"], mesh.shape["ctx"])),
        mesh=mesh,
        in_specs=placed,
        out_specs=(P("dp", "ctx", None), P("dp", "ctx", None), P("dp", None, "ctx")),
        check_vma=False,
    )
```

```python
import functools
import math

import jax
import jax.numpy as jnp
from jax import lax
from jax.experimental import pallas as pl
from jax.experimental.pallas import tpu as pltpu
from jax.sharding import PartitionSpec as P

HEAD = 128


def dot(a, b, dims):
    return lax.dot_general(a, b, (dims, ((), ())), preferred_element_type=jnp.float32)


def attend_block(block, bias_ref, q_ref, g_ref, kv_ref, out_ref, gq_ref, gkv_ref):
    scale = 1.0 / math.sqrt(HEAD)
    bias = bias_ref[...]
    heads = kv_ref.shape[2] // (2 * HEAD)
    for h in range(heads):
        own = pl.ds(pl.multiple_of((block * heads + h) * HEAD, HEAD), HEAD)
        at_key = slice(2 * h * HEAD, (2 * h + 1) * HEAD)
        at_value = slice((2 * h + 1) * HEAD, (2 * h + 2) * HEAD)
        q = q_ref[:, own]
        g = g_ref[:, own]
        key = kv_ref[block, :, at_key]
        value = kv_ref[block, :, at_value]
        scores = dot(q, key, ((1,), (1,))) * scale + bias
        top = jnp.max(scores, axis=-1, keepdims=True)
        weights = jnp.exp(scores - top)
        probs = weights * (1.0 / jnp.sum(weights, axis=-1, keepdims=True))
        probs_low = probs.astype(jnp.bfloat16)
        out_ref[:, own] = dot(probs_low, value, ((1,), (0,))).astype(jnp.bfloat16)
        grad_probs = dot(g, value, ((1,), (1,)))
        delta = jnp.sum(probs * grad_probs, axis=-1, keepdims=True)
        grad_scores = (probs * (grad_probs - delta) * scale).astype(jnp.bfloat16)
        gq_ref[:, own] = dot(grad_scores, key, ((1,), (0,))).astype(jnp.bfloat16)
        gkv_ref[block, :, at_key] = dot(grad_scores, q, ((0,), (0,))).astype(gkv_ref.dtype)
        gkv_ref[block, :, at_value] = dot(probs_low, g, ((0,), (0,))).astype(gkv_ref.dtype)


def greet(axis, a, last, up, down, partner):
    barrier = pltpu.get_barrier_semaphore()

    def hello(target):
        pl.semaphore_signal(barrier, inc=1, device_id={axis: target}, device_id_type=pl.DeviceIdType.MESH)

    hello(partner)

    @pl.when(a < last)
    def _():
        hello(up)

    @pl.when(a > 0)
    def _():
        hello(down)

    if last == 0:
        pl.semaphore_wait(barrier, 1)
    else:
        @pl.when((a > 0) & (a < last))
        def _():
            pl.semaphore_wait(barrier, 3)

        @pl.when((a == 0) | (a == last))
        def _():
            pl.semaphore_wait(barrier, 2)


def gather_kernel(axis, n, own_ref, out_ref, own_sem, send_sems, recv_sems):
    me = lax.axis_index(axis)
    a, b = me // 2, me % 2
    last = n // 2 - 1
    up, down, partner = me + 2, me - 2, a * 2 + (1 - b)
    greet(axis, a, last, up, down, partner)
    mine = pltpu.make_async_copy(own_ref, out_ref.at[me], own_sem)
    mine.start()

    def hop(source, block, way, target):
        return pltpu.make_async_remote_copy(
            src_ref=source, dst_ref=out_ref.at[block], send_sem=send_sems.at[block, way],
            recv_sem=recv_sems.at[block], device_id={axis: target}, device_id_type=pl.DeviceIdType.MESH,
        )

    @pl.when(a < last)
    def _():
        hop(own_ref, me, 0, up).start()

    @pl.when(a > 0)
    def _():
        hop(own_ref, me, 1, down).start()

    hop(own_ref, me, 2, partner).start()
    for s in range(1, last + 1):
        @pl.when(a >= s)
        def _():
            block = (a - s) * 2 + b
            hop(own_ref, block, 0, partner).wait_recv()

            @pl.when(a < last)
            def _():
                hop(out_ref.at[block], block, 0, up).start()

            hop(out_ref.at[block], block, 2, partner).start()

        @pl.when(a + s <= last)
        def _():
            block = (a + s) * 2 + b
            hop(own_ref, block, 1, partner).wait_recv()

            @pl.when(a > 0)
            def _():
                hop(out_ref.at[block], block, 1, down).start()

            hop(out_ref.at[block], block, 2, partner).start()

    for z in range(last + 1):
        hop(own_ref, z * 2 + 1 - b, 2, partner).wait_recv()
        hop(own_ref, z * 2 + b, 2, partner).wait_send()

        @pl.when((a < last) & (a >= z))
        def _():
            hop(own_ref, z * 2 + b, 0, partner).wait_send()

        @pl.when((a > 0) & (a <= z))
        def _():
            hop(own_ref, z * 2 + b, 1, partner).wait_send()

    mine.wait()


def gather(block, axis, n, collective_id):
    return pl.pallas_call(
        functools.partial(gather_kernel, axis, n),
        in_specs=[pl.BlockSpec(memory_space=pltpu.VMEM)],
        out_specs=pl.BlockSpec(memory_space=pl.ANY),
        out_shape=jax.ShapeDtypeStruct((n,) + block.shape, block.dtype),
        scratch_shapes=[
            pltpu.SemaphoreType.DMA,
            pltpu.SemaphoreType.DMA((n, 3)),
            pltpu.SemaphoreType.DMA((n,)),
        ],
        compiler_params=pltpu.CompilerParams(collective_id=collective_id, has_side_effects=True),
        name="gather",
    )(block)


def scatter_kernel(axis, n, compute, g_ref, out_ref, crossed, risen, fallen, going, send_sems, x_sems, up_sems, down_sems):
    me = lax.axis_index(axis)
    a, b = me // 2, me % 2
    last = n // 2 - 1
    up, down, partner = me + 2, me - 2, a * 2 + (1 - b)
    greet(axis, a, last, up, down, partner)
    rows = out_ref.shape[0]
    step = min(rows, 32)
    half = (last + 2) // 2
    high = a // half

    def place(t):
        return high * t + (1 - high) * (last - t)

    def cross(z):
        return pltpu.make_async_remote_copy(
            src_ref=g_ref.at[z * 2 + 1 - b], dst_ref=crossed.at[z], send_sem=send_sems.at[z, 0],
            recv_sem=x_sems.at[z], device_id={axis: partner}, device_id_type=pl.DeviceIdType.MESH,
        )

    def rise(z):
        return pltpu.make_async_remote_copy(
            src_ref=going.at[z], dst_ref=risen.at[z], send_sem=send_sems.at[z, 1],
            recv_sem=up_sems.at[z], device_id={axis: up}, device_id_type=pl.DeviceIdType.MESH,
        )

    def fall(z):
        return pltpu.make_async_remote_copy(
            src_ref=going.at[z], dst_ref=fallen.at[z], send_sem=send_sems.at[z, 2],
            recv_sem=down_sems.at[z], device_id={axis: down}, device_id_type=pl.DeviceIdType.MESH,
        )

    def add(target, parts):
        @pl.loop(0, rows // step)
        def _(i):
            at = pl.ds(pl.multiple_of(i * step, step), step)
            total = parts[0][at, :].astype(jnp.float32)
            for part in parts[1:]:
                total = total + part[at, :].astype(jnp.float32)
            target[at, :] = total.astype(target.dtype)

    if compute is None:
        for t in range(last + 1):
            cross(place(t)).start()
    else:
        @pl.loop(0, last + 1)
        def _(t):
            compute(place(t) * 2 + 1 - b)
            cross(place(t)).start()

        @pl.loop(0, last + 1)
        def _(t):
            compute(place(t) * 2 + b)

    for t in range(last + 1):
        z = place(t)
        cross(z).wait_recv()
        pair = [g_ref.at[z * 2 + b], crossed.at[z]]

        @pl.when(z > a)
        def _():
            @pl.when(a > 0)
            def _():
                rise(z).wait_recv()
                add(going.at[z], pair + [risen.at[z]])

            @pl.when(a == 0)
            def _():
                add(going.at[z], pair)

            rise(z).start()

        @pl.when(z < a)
        def _():
            @pl.when(a < last)
            def _():
                fall(z).wait_recv()
                add(going.at[z], pair + [fallen.at[z]])

            @pl.when(a == last)
            def _():
                add(going.at[z], pair)

            fall(z).start()

    pair = [g_ref.at[a * 2 + b], crossed.at[a]]

    @pl.when(a > 0)
    def _():
        rise(a).wait_recv()

    @pl.when(a < last)
    def _():
        fall(a).wait_recv()

    @pl.when(a == 0)
    def _():
        add(out_ref, pair + [fallen.at[a]])

    @pl.when(a == last)
    def _():
        add(out_ref, pair + [risen.at[a]])

    @pl.when((a > 0) & (a < last))
    def _():
        add(out_ref, pair + [risen.at[a], fallen.at[a]])

    for z in range(last + 1):
        cross(z).wait_send()

        @pl.when(z > a)
        def _():
            rise(z).wait_send()

        @pl.when(z < a)
        def _():
            fall(z).wait_send()


def scatter(parts, axis, collective_id):
    n, rows, columns = parts.shape
    half = n // 2
    blocks = pltpu.VMEM((half, rows, columns), parts.dtype)
    return pl.pallas_call(
        functools.partial(scatter_kernel, axis, n, None),
        in_specs=[pl.BlockSpec(memory_space=pltpu.VMEM)],
        out_specs=pl.BlockSpec(memory_space=pltpu.VMEM),
        out_shape=jax.ShapeDtypeStruct((rows, columns), jnp.bfloat16),
        scratch_shapes=[blocks] * 4
        + [
            pltpu.SemaphoreType.DMA((half, 3)),
            pltpu.SemaphoreType.DMA((half,)),
            pltpu.SemaphoreType.DMA((half,)),
            pltpu.SemaphoreType.DMA((half,)),
        ],
        compiler_params=pltpu.CompilerParams(
            collective_id=collective_id, has_side_effects=True, vmem_limit_bytes=40 << 20
        ),
        name="scatter",
    )(parts)


def attend_kernel(axis, n, bias_ref, q_ref, g_ref, kv_ref, out_ref, gq_ref, sum_ref, gkv_ref, *rest):
    def compute(block):
        attend_block(block, bias_ref, q_ref, g_ref, kv_ref, out_ref, gq_ref, gkv_ref)

    scatter_kernel(axis, n, compute, gkv_ref, sum_ref, *rest)


def attend(bias, queries, grad_out, kv, axis, collective_id):
    n, rows, columns = kv.shape
    half = n // 2
    blocks = pltpu.VMEM((half, rows, columns), jnp.bfloat16)
    vmem = pl.BlockSpec(memory_space=pltpu.VMEM)
    return pl.pallas_call(
        functools.partial(attend_kernel, axis, n),
        in_specs=[vmem] * 4,
        out_specs=[vmem] * 3,
        out_shape=[
            jax.ShapeDtypeStruct(queries.shape, jnp.bfloat16),
            jax.ShapeDtypeStruct(queries.shape, jnp.bfloat16),
            jax.ShapeDtypeStruct((rows, columns), jnp.bfloat16),
        ],
        scratch_shapes=[pltpu.VMEM(kv.shape, jnp.bfloat16)]
        + [blocks] * 4
        + [
            pltpu.SemaphoreType.DMA((half, 3)),
            pltpu.SemaphoreType.DMA((half,)),
            pltpu.SemaphoreType.DMA((half,)),
            pltpu.SemaphoreType.DMA((half,)),
        ],
        compiler_params=pltpu.CompilerParams(
            collective_id=collective_id, has_side_effects=True, vmem_limit_bytes=48 << 20
        ),
        name="attend",
    )(bias, queries, grad_out, kv)


def per_device(groups, text, src, lengths, kv_weight, queries, grad_out):
    dp, ctx = groups
    group = lax.axis_index("dp")
    samples = src.shape[0]
    share = ctx // dp
    tokens = text.shape[2]
    keys = 2 * tokens
    features = kv_weight.shape[0]
    columns = kv_weight.shape[2]
    hops = [
        (d * ctx + c, (c // share) * ctx + d * share + c % share)
        for d in range(dp)
        for c in range(ctx)
    ]
    mine = lax.ppermute(text[0], ("dp", "ctx"), hops)
    pieces = gather(mine.reshape(2 * tokens, -1), "ctx", ctx, 1)
    pieces = pieces.reshape(samples, share, 2, tokens, features // share)
    by_text = jnp.transpose(pieces, (0, 2, 3, 1, 4)).reshape(samples, 2, tokens, features)
    rows = jnp.stack(
        [lax.dynamic_index_in_dim(by_text, src[b], 0, keepdims=False) for b in range(samples)]
    )
    partial = jnp.einsum("betf,fec->betc", rows, kv_weight, preferred_element_type=jnp.float32)
    kv_local = scatter(partial.reshape(samples, keys, columns), "dp", 4)
    kv = gather(kv_local, "ctx", ctx, 2)
    own_lengths = lax.dynamic_index_in_dim(lengths, src[group], 0, keepdims=False)
    valid = jnp.arange(tokens, dtype=jnp.int32)[None, :] < own_lengths[:, None]
    bias = jnp.where(valid, 0.0, -1e30).astype(jnp.float32).reshape(1, keys)
    attended, grad_queries, grad_low = attend(bias, queries[0], grad_out[0], kv, "ctx", 3)
    grads = gather(grad_low, "dp", dp, 5)
    grads = grads.reshape(samples, 2, tokens, columns)
    grad_weight = jnp.einsum("betf,betc->fec", rows, grads, preferred_element_type=jnp.float32)
    return (attended[None], grad_queries[None], grad_weight)


def solution(mesh):
    placed = (
        P("dp", None, None, "ctx"),
        P(),
        P(),
        P("dp", None, "ctx"),
        P("dp", "ctx", None),
        P("dp", "ctx", None),
    )
    return jax.shard_map(
        functools.partial(per_device, (mesh.shape["dp"], mesh.shape["ctx"])),
        mesh=mesh,
        in_specs=placed,
        out_specs=(P("dp", "ctx", None), P("dp", "ctx", None), P("dp", None, "ctx")),
        check_vma=False,
    )
```
